32 devices in a mesh: section: 2 (over x), blk: 8 (over z, y), head: 2 (over core).
Axes of the slice: x: 2, y: 2, z: 4, core: 2. Of those that a mesh axis runs over, the one named last changes fastest.
Arguments:
- hidden_in: bfloat16 [4, 64, 1536], P(None, 'blk', 'head'), may hold values from -6 to 6
- w_qkv: bfloat16 [2, 1536, 3, 1536], P('section', 'blk', None, 'head'), may hold values from -0.15625 to 0.15625
- norm_gain: float32 [2, 1536], P('section'), may hold values from 0.5 to 1.5
- qk_gain: float32 [2, 2, 128], P('section'), may hold values from 1 to 2
- text_states: bfloat16 [2, 256, 1536], P('section'), may hold values from -6 to 6
- text_len: int32 [1], replicated, may hold values from 64 to 256
- patch_len: int32 [4], replicated, may hold values from 32 to 64
- stale_flags: int32 [4, 2], replicated, may hold values from 0 to 1, as said below
- stale_kv: bfloat16 [2, 2, 4, 64, 1536], P('section', None, None, 'blk', 'head'), may hold values from -6 to 6
Outputs:
- hidden_out: bfloat16 [2, 4, 64, 1536], P('section', None, 'blk', 'head')
- new_cache: bfloat16 [2, 2, 4, 64, 1536], P('section', None, None, 'blk', 'head')
The draws below stay inside these ranges and needn't reach their ends.
Inputs may be any that keep to these rules, and one draw needn't show every extreme that they name: `stale_flags`: 1 means that the micro-batch uses the previous step's keys and values at that layer, 0 that it uses its fresh ones; every layer has at least one micro-batch flagged 1 and at least one flagged 0.
All inputs are finite; a program needn't handle non-finite values.
Results may differ from the reference program's by a relative error of at most 0.02.
Values may be sent and summed in bfloat16 or wider, within the bound.
A program may use at most 64 MiB of HBM per device.

```python
import math
import jax
import jax.numpy as jnp
from jax import lax

D = 1536
HEADS = 12
HEAD_DIM = 128
TEXT = 256
MICRO = 4
LAYERS = 2
PATCH = 64


def draw_stale_flags(key, part):
    bits_key = jax.random.fold_in(key, 101)
    pick_key = jax.random.fold_in(key, 202)
    random_bits = jax.random.randint(bits_key, (MICRO, LAYERS), 0, 2).astype(jnp.int32)
    chosen = jax.random.randint(pick_key, (1, LAYERS), 0, MICRO).astype(jnp.int32)
    rows = jnp.arange(MICRO, dtype=jnp.int32)[:, None]
    forced_on = rows == chosen
    forced_off = rows == (chosen + 1) % MICRO
    flags = jnp.where(forced_on, 1, jnp.where(forced_off, 0, random_bits))
    return flags.astype(jnp.int32)


def plant(array, own_key, low, high):
    spot = [jax.random.randint(jax.random.fold_in(own_key, axis), (), 0, length) for axis, length in enumerate(array.shape)]
    main_axis = array.shape.index(max(array.shape))
    next_to = spot[:main_axis] + [(spot[main_axis] + 1) % array.shape[main_axis]] + spot[main_axis + 1:]
    return array.at[tuple(spot)].set(low).at[tuple(next_to)].set(high)


def levels(rng, extent, pieces, smallest, top_value):
    def one(dim, parts):
        steps = jax.random.uniform(jax.random.fold_in(jax.random.fold_in(rng, 6), dim), (parts,), jnp.float32, smallest / len(pieces), top_value / len(pieces))
        return jnp.repeat(jnp.exp(steps), extent[dim] // parts).reshape((-1,) + (1,) * (len(extent) - dim - 1))

    loudness = one(*pieces[0])
    for cut in pieces[1:]:
        loudness = loudness * one(*cut)
    return loudness


def gaussian(own_key, dims, scale, reach, split=(), kind=jnp.bfloat16):
    result = jax.random.normal(own_key, dims, jnp.float32) * scale
    if len(split) > 0:
        result = levels(own_key, dims, split, -0.22, 0.18) * result
    return jnp.clip(result, min=-reach, max=reach).astype(kind)


def setup_inputs(seed: int = 0) -> dict:
    splits = jax.random.split(jax.random.key(seed), 10)
    hidden_in = gaussian(splits[0], (MICRO, PATCH, D), 1.0, 6.0, ((1, 8), (2, 2)))
    w_qkv = gaussian(splits[1], (LAYERS, D, 3, HEADS * HEAD_DIM), D ** -0.5, 0.15625, ((0, 2), (1, 8), (3, 2)))
    norm_gain = jnp.clip(1.0 + 0.1 * jax.random.normal(splits[2], (LAYERS, D), jnp.float32), 0.5, 1.5)
    qk_gain = jnp.clip(jnp.exp(math.log(2.0) - 0.6931472 * jax.random.uniform(splits[3], (LAYERS, 2, HEAD_DIM), jnp.float32) ** levels(splits[3], (LAYERS, 2, HEAD_DIM), ((0, 2),), -0.2, 0.2)), 1.0, 2.0)
    text_states = gaussian(splits[4], (LAYERS, TEXT, D), 1.0, 6.0, ((0, 2),))
    text_len = jax.random.randint(splits[5], (1,), TEXT // 4, TEXT + 1).astype(jnp.int32)
    patch_len = plant(jax.random.randint(splits[6], (MICRO,), PATCH // 2, PATCH + 1), jax.random.fold_in(splits[6], 1), PATCH // 2, PATCH).astype(jnp.int32)
    stale_flags = draw_stale_flags(jax.random.fold_in(splits[9], 71), 0)
    stale_kv = gaussian(splits[8], (LAYERS, 2, MICRO, PATCH, HEADS * HEAD_DIM), 1.0, 6.0, ((0, 2), (3, 8), (4, 2)))
    return dict(hidden_in=hidden_in, w_qkv=w_qkv, norm_gain=norm_gain, qk_gain=qk_gain, text_states=text_states, text_len=text_len, patch_len=patch_len, stale_flags=stale_flags, stale_kv=stale_kv)


def norm_rows(values, row_gain):
    return values * lax.rsqrt(lax.optimization_barrier(jnp.mean(values * values, axis=-1, keepdims=True)) + 1e-06) * row_gain

def attend_part(queries, key_rows, value_rows, key_mask):
    scores = jnp.einsum('qhd,khd->hqk', queries.astype(jnp.float32), key_rows.astype(jnp.float32), precision=lax.Precision.HIGHEST) * HEAD_DIM ** (-0.5)
    probs = jnp.where(key_mask[None, None, :], jnp.exp(scores), 0.0)
    numerator = jnp.einsum('hqk,khd->qhd', probs.astype(jnp.bfloat16).astype(jnp.float32), value_rows.astype(jnp.float32), precision=lax.Precision.HIGHEST)
    return (numerator, lax.optimization_barrier(jnp.sum(probs, axis=2)))

def reference(hidden_in, w_qkv, norm_gain, qk_gain, text_states, text_len, patch_len, stale_flags, stale_kv):
    width = HEADS * HEAD_DIM
    text_mask = jnp.arange(TEXT) < text_len[0]
    positions = jnp.arange(PATCH)
    state_all = hidden_in
    hidden_layers = []
    cache_layers = []
    for layer_idx in range(LAYERS):
        weight_flat = w_qkv[layer_idx].reshape(D, 3 * width)
        row_gain = norm_gain[layer_idx]
        query_gain = qk_gain[layer_idx, 0]
        key_gain = qk_gain[layer_idx, 1]
        text_normed = norm_rows(text_states[layer_idx].astype(jnp.float32), row_gain).astype(jnp.bfloat16)
        text_kv = jnp.dot(text_normed, weight_flat[:, width:], preferred_element_type=jnp.float32).astype(jnp.bfloat16)
        text_kv = text_kv.reshape(TEXT, 2, HEADS, HEAD_DIM)
        text_keys = norm_rows(text_kv[:, 0].astype(jnp.float32), key_gain).astype(jnp.bfloat16)
        text_values = text_kv[:, 1]
        layer_hidden = []
        layer_cache = []
        for micro_idx in range(MICRO):
            rows_in = state_all[micro_idx]
            normed = norm_rows(rows_in.astype(jnp.float32), row_gain).astype(jnp.bfloat16)
            projected = jnp.dot(normed, weight_flat, preferred_element_type=jnp.float32).reshape(PATCH, 3, width)
            fresh_kv = jnp.moveaxis(projected[:, 1:], 1, 0).astype(jnp.bfloat16)
            kept_kv = jnp.where(stale_flags[micro_idx, layer_idx] == 1, stale_kv[layer_idx, :, micro_idx], fresh_kv)
            key_rows = norm_rows(kept_kv[0].astype(jnp.float32).reshape(PATCH, HEADS, HEAD_DIM), key_gain).astype(jnp.bfloat16)
            value_rows = kept_kv[1].reshape(PATCH, HEADS, HEAD_DIM)
            queries = norm_rows(projected[:, 0].reshape(PATCH, HEADS, HEAD_DIM), query_gain).astype(jnp.bfloat16)
            text_num, text_den = attend_part(queries, text_keys, text_values, text_mask)
            own_num, own_den = attend_part(queries, key_rows, value_rows, positions < patch_len[micro_idx])
            attended = (text_num + own_num) / jnp.transpose(text_den + own_den)[:, :, None]
            layer_hidden.append((rows_in.astype(jnp.float32) + attended.reshape(PATCH, width)).astype(jnp.bfloat16))
            layer_cache.append(fresh_kv)
        state_all = jnp.stack(layer_hidden)
        hidden_layers.append(state_all)
        cache_layers.append(jnp.stack(layer_cache, axis=1))
    return (jnp.stack(hidden_layers), jnp.stack(cache_layers))
```

```python
import functools

import jax
import jax.numpy as jnp
from jax import lax
from jax.experimental import pallas as pl
from jax.experimental.pallas import tpu as pltpu
from jax.sharding import PartitionSpec as P

MESH = pl.DeviceIdType.MESH
F32 = jnp.float32
BF16 = jnp.bfloat16


def rms(values, gain):
    return values * lax.rsqrt(jnp.mean(values * values, axis=-1, keepdims=True) + 1e-06) * gain


def kernel(
    dims,
    text_len, patch_len, flags,
    hid_in, w_in, row_gain, head_gain, text_in, stale_in,
    hid_out, cache_out,
    X, XN, TN, W, ST, TK, TV, hid_own, cache_own,
    zs, zr, ys, yr, ws, wr, ss, sr, hs, hr, cs, cr, one,
):
    S, B, heads, hd, micro, tok = dims
    off = (B - heads) // 2
    rows = micro * tok
    total = B * rows
    width = heads * hd
    depth = w_in.shape[1]
    s, b, h = lax.axis_index("section"), lax.axis_index("blk"), lax.axis_index("head")
    mate = b + 1 - 2 * lax.rem(b, 2)
    j_own = b - off
    owner = (b >= off) & (b < off + heads)
    half = pl.ds(pl.multiple_of(h * width, hd), width)
    other_half = pl.ds(pl.multiple_of((1 - h) * width, hd), width)

    def ahead(k):
        return lax.rem(b + k, B)

    def remote(src, dst, send, recv, dev):
        return pltpu.make_async_remote_copy(
            src_ref=src, dst_ref=dst, send_sem=send, recv_sem=recv, device_id=dev, device_id_type=MESH
        )

    def arrived(dst, sem):
        pltpu.make_async_copy(dst, dst, sem).wait()

    def push(src, dst, send, recv, target):
        @pl.when(target == b)
        def _():
            pltpu.make_async_copy(src, dst, recv).start()

        @pl.when(target != b)
        def _():
            remote(src, dst, send, recv, (s, target, h)).start()

    def pushed(src, send, target):
        @pl.when(target != b)
        def _():
            remote(src, src, send, send, (s, target, h)).wait_send()

    barrier = pltpu.get_barrier_semaphore()
    for k in range(1, B):
        pl.semaphore_signal(barrier, inc=1, device_id=(s, ahead(k), h), device_id_type=MESH)
    pl.semaphore_signal(barrier, inc=1, device_id=(s, b, 1 - h), device_id_type=MESH)

    @pl.when(s > 0)
    def _():
        pl.semaphore_signal(barrier, inc=1, device_id=(s - 1, b, h), device_id_type=MESH)

    @pl.when(s < S - 1)
    def _():
        pl.semaphore_signal(barrier, inc=1, device_id=(s + 1, b, h), device_id_type=MESH)

    pl.semaphore_wait(barrier, B + (s > 0).astype(jnp.int32) + (s < S - 1).astype(jnp.int32))

    def row_block(c):
        return X.at[c, :, half]

    def col_block(j):
        return X.at[:, :, pl.ds(pl.multiple_of(h * width + j * hd, hd), hd)]

    swap_cores = lambda: remote(X.at[:, :, half], X.at[:, :, half], one.at[0], one.at[1], (s, b, 1 - h))
    swap_in = lambda: arrived(X.at[:, :, other_half], one.at[1])

    @pl.when(s == 0)
    def _():
        pltpu.make_async_copy(hid_in, row_block(b), one.at[2]).start()
        for k in range(2, B, 2):
            remote(hid_in, row_block(b), zs.at[k], zr.at[b], (s, ahead(k), h)).start()
        remote(hid_in, row_block(b), ys.at[0], yr.at[b], (s, mate, h)).start()

    w_dst = W.at[pl.ds(pl.multiple_of(b * depth, depth), depth), :]
    st_dst = ST.at[:, b]
    for k in range(heads):
        j = lax.rem(b + k, heads)
        push(w_in.at[j], w_dst, ws.at[k], wr.at[b], j + off)
        st_src = stale_in.at[:, :, pl.ds(pl.multiple_of(j * hd, hd), hd)]
        push(st_src, st_dst, ss.at[k], sr.at[b], j + off)

    def norm_states():
        values = X[...].reshape(total, 2 * width).astype(F32)
        XN[...] = rms(values, row_gain[...]).astype(BF16)

    @pl.when(s == 0)
    def _():
        for k in range(2, B, 2):
            c = ahead(k)
            arrived(row_block(c), zr.at[c])
            remote(row_block(c), row_block(c), ys.at[k], yr.at[c], (s, mate, h)).start()
        pltpu.make_async_copy(hid_in, row_block(b), one.at[2]).wait()
        for k in range(0, B, 2):
            c = lax.rem(mate + k, B)
            arrived(row_block(c), yr.at[c])
        swap_cores().start()
        swap_in()

        @pl.when(owner)
        def _():
            norm_states()

    @pl.when(owner)
    def _():
        TN[...] = rms(text_in[...].astype(F32), row_gain[...]).astype(BF16)
        for c in range(B):
            arrived(W.at[pl.ds(c * depth, depth), :], wr.at[c])
        text_kv = jnp.dot(TN[...], W[:, hd:], preferred_element_type=F32).astype(BF16)
        TK[...] = rms(text_kv[:, :hd].astype(F32), head_gain[1:2, :]).astype(BF16)
        TV[...] = text_kv[:, hd:]
        for c in range(B):
            arrived(ST.at[:, c], sr.at[c])

    @pl.when(s > 0)
    def _():
        @pl.when(owner)
        def _():
            mine = col_block(j_own)
            arrived(mine, one.at[3])
            for k in range(2, B, 2):
                remote(mine, mine, zs.at[k], zr.at[b], (s, ahead(k), h)).start()
            remote(mine, mine, ys.at[0], yr.at[b], (s, mate, h)).start()

        for k in range(2, B, 2):
            c = ahead(k)

            @pl.when((c >= off) & (c < off + heads))
            def _():
                block = col_block(c - off)
                arrived(block, zr.at[c])
                remote(block, block, ys.at[k], yr.at[c], (s, mate, h)).start()

        for k in range(0, B, 2):
            c = lax.rem(mate + k, B)

            @pl.when((c >= off) & (c < off + heads))
            def _():
                arrived(col_block(c - off), yr.at[c])

        swap_cores().start()
        swap_in()

        @pl.when(owner)
        def _():
            norm_states()

    @pl.when(owner)
    def _():
        proj = jnp.dot(XN[...], W[...], preferred_element_type=F32)
        fresh_k = proj[:, hd : 2 * hd].astype(BF16)
        fresh_v = proj[:, 2 * hd :].astype(BF16)
        cache_own[0] = fresh_k.reshape(B, rows, hd)
        cache_own[1] = fresh_v.reshape(B, rows, hd)
        tok_bits = tok.bit_length() - 1

        def place(shape, axis):
            at = lax.broadcasted_iota(jnp.int32, shape, axis)
            which = lax.shift_right_logical(at, tok_bits) & (micro - 1)
            spot = lax.shift_right_logical(at, rows.bit_length() - 1) * tok + (at & (tok - 1))
            return which, spot

        def per_micro(which, read):
            out = jnp.zeros(which.shape, jnp.int32)
            for m in range(micro):
                out = jnp.where(which == m, read(m), out)
            return out

        which, _ = place((total, hd), 0)
        use_stale = per_micro(which, lambda m: flags[m, s]) == 1
        kept_k = jnp.where(use_stale, ST[0].reshape(total, hd).astype(F32), fresh_k.astype(F32))
        kept_v = jnp.where(use_stale, ST[1].reshape(total, hd).astype(F32), fresh_v.astype(F32))
        keys = rms(kept_k, head_gain[1:2, :]).astype(BF16)
        queries = rms(proj[:, :hd], head_gain[0:1, :]).astype(BF16)
        scale = hd**-0.5
        nt = (((1,), (1,)), ((), ()))

        def attend(key_rows, value_rows, mask):
            scores = lax.dot_general(queries, key_rows, nt, preferred_element_type=F32) * scale
            probs = jnp.where(mask, jnp.exp(scores), 0.0)
            num = jnp.dot(probs.astype(BF16), value_rows, preferred_element_type=F32)
            return num, jnp.sum(probs, axis=1, keepdims=True)

        shape = (total, total)
        q_which, _ = place(shape, 0)
        k_which, k_spot = place(shape, 1)
        mask = (q_which == k_which) & (k_spot < per_micro(k_which, lambda m: patch_len[m]))
        num, den = attend(keys, kept_v.astype(BF16), mask)
        text_at = lax.broadcasted_iota(jnp.int32, (total, TK.shape[0]), 1)
        text_num, text_den = attend(TK[...], TV[...], text_at < text_len[0])
        attended = (num + text_num) / (den + text_den)
        state = X[:, :, pl.ds(pl.multiple_of(h * width + j_own * hd, hd), hd)]
        new = (state.reshape(total, hd).astype(F32) + attended).astype(BF16)
        hid_own[...] = new.reshape(B, rows, hd)

        @pl.when(s < S - 1)
        def _():
            remote(hid_own, col_block(j_own), one.at[4], one.at[3], (s + 1, b, h)).start()

        cols = pl.ds(pl.multiple_of(j_own * hd, hd), hd)
        for k in range(B):
            t = ahead(k)
            push(hid_own.at[t], hid_out.at[:, cols], hs.at[k], hr.at[j_own], t)
            push(cache_own.at[:, t], cache_out.at[:, :, cols], cs.at[k], cr.at[j_own], t)
        for k in range(B):
            t = ahead(k)
            pushed(hid_own.at[t], hs.at[k], t)
            pushed(cache_own.at[:, t], cs.at[k], t)

        @pl.when(s < S - 1)
        def _():
            remote(hid_own, col_block(j_own), one.at[4], one.at[3], (s + 1, b, h)).wait_send()

    for j in range(heads):
        cols = pl.ds(j * hd, hd)
        arrived(hid_out.at[:, cols], hr.at[j])
        arrived(cache_out.at[:, :, cols], cr.at[j])

    for k in range(heads):
        j = lax.rem(b + k, heads)
        pushed(w_in.at[j], ws.at[k], j + off)
        pushed(stale_in.at[:, :, pl.ds(pl.multiple_of(j * hd, hd), hd)], ss.at[k], j + off)
    swap_cores().wait_send()

    @pl.when(s == 0)
    def _():
        for k in range(2, B, 2):
            remote(hid_in, row_block(b), zs.at[k], zr.at[b], (s, ahead(k), h)).wait_send()
        for k in range(0, B, 2):
            remote(hid_in, row_block(b), ys.at[k], yr.at[b], (s, mate, h)).wait_send()

    @pl.when(s > 0)
    def _():
        block = col_block(0)

        @pl.when(owner)
        def _():
            for k in range(2, B, 2):
                remote(block, block, zs.at[k], zr.at[b], (s, ahead(k), h)).wait_send()

        for k in range(0, B, 2):
            c = ahead(k)

            @pl.when((c >= off) & (c < off + heads))
            def _():
                remote(block, block, ys.at[k], yr.at[b], (s, mate, h)).wait_send()


def shards(
    hidden_in, w_qkv, norm_gain, qk_gain, text_states, text_len, patch_len, stale_flags, stale_kv
):
    S, B = lax.axis_size("section"), lax.axis_size("blk")
    micro, tok, width = hidden_in.shape
    hd = qk_gain.shape[2]
    heads = width // hd
    rows = micro * tok
    total = B * rows
    depth = w_qkv.shape[1]
    text = text_states.shape[1]
    w = w_qkv[0].reshape(depth, 3, heads, hd).transpose(2, 0, 1, 3).reshape(heads, depth, 3 * hd)
    smem = pl.BlockSpec(memory_space=pltpu.SMEM)
    vmem = pl.BlockSpec(memory_space=pltpu.VMEM)
    sem = pltpu.SemaphoreType.DMA
    hid, cache = pl.pallas_call(
        functools.partial(kernel, (S, B, heads, hd, micro, tok)),
        out_shape=(
            jax.ShapeDtypeStruct((rows, width), BF16),
            jax.ShapeDtypeStruct((2, rows, width), BF16),
        ),
        in_specs=[smem] * 3 + [vmem] * 6,
        out_specs=(vmem, vmem),
        scratch_shapes=[
            pltpu.VMEM((B, rows, 2 * width), BF16),
            pltpu.VMEM((total, 2 * width), BF16),
            pltpu.VMEM((text, 2 * width), BF16),
            pltpu.VMEM((B * depth, 3 * hd), BF16),
            pltpu.VMEM((2, B, rows, hd), BF16),
            pltpu.VMEM((text, hd), BF16),
            pltpu.VMEM((text, hd), BF16),
            pltpu.VMEM((B, rows, hd), BF16),
            pltpu.VMEM((2, B, rows, hd), BF16),
            sem((B,)), sem((B,)), sem((B,)), sem((B,)),
            sem((heads,)), sem((B,)), sem((heads,)), sem((B,)),
            sem((B,)), sem((heads,)), sem((B,)), sem((heads,)),
            sem((5,)),
        ],
        compiler_params=pltpu.CompilerParams(
            collective_id=0, has_side_effects=True, vmem_limit_bytes=60 * 1024 * 1024
        ),
    )(
        text_len, patch_len, stale_flags,
        hidden_in.reshape(rows, width), w, norm_gain, qk_gain[0], text_states[0],
        stale_kv[0].reshape(2, rows, width),
    )
    return (
        hid.reshape(1, micro, tok, width),
        cache.reshape(1, 2, micro, tok, width),
    )


def solution(mesh):
    in_specs = (
        P(None, "blk", "head"),
        P("section", "blk", None, "head"),
        P("section", None),
        P("section", None, None),
        P("section", None, None),
        P(),
        P(),
        P(),
        P("section", None, None, "blk", "head"),
    )
    out_specs = (P("section", None, "blk", "head"), P("section", None, None, "blk", "head"))
    return jax.shard_map(shards, mesh=mesh, in_specs=in_specs, out_specs=out_specs, check_vma=False)
```

```python
import functools

import jax
import jax.numpy as jnp
from jax import lax
from jax.experimental import pallas as pl
from jax.experimental.pallas import tpu as pltpu
from jax.sharding import PartitionSpec as P

MESH = pl.DeviceIdType.MESH
F32 = jnp.float32
BF16 = jnp.bfloat16


def rms(values, gain):
    return values * lax.rsqrt(jnp.mean(values * values, axis=-1, keepdims=True) + 1e-06) * gain


def kernel(
    dims,
    text_len, patch_len, flags,
    hid_in, w_in, row_gain, head_gain, text_in, stale_in,
    hid_out, cache_out,
    X, G, XN, TN, W, ST, TK, TV, hid_own, cache_own,
    zs, zr, ys, yr, ws, wr, ss, sr, hs, hr, cs, cr, gzs, gzr, gys, gyr, gxs, one,
):
    S, B, heads, hd, micro, tok = dims
    off = (B - heads) // 2
    rows = micro * tok
    total = B * rows
    width = heads * hd
    depth = w_in.shape[1]
    s, b, h = lax.axis_index("section"), lax.axis_index("blk"), lax.axis_index("head")
    mate = b + 1 - 2 * lax.rem(b, 2)
    j_own = b - off
    owner = (b >= off) & (b < off + heads)
    half = pl.ds(pl.multiple_of(h * width, hd), width)
    other_half = pl.ds(pl.multiple_of((1 - h) * width, hd), width)

    def ahead(k):
        return lax.rem(b + k, B)

    def remote(src, dst, send, recv, dev):
        return pltpu.make_async_remote_copy(
            src_ref=src, dst_ref=dst, send_sem=send, recv_sem=recv, device_id=dev, device_id_type=MESH
        )

    def arrived(dst, sem):
        pltpu.make_async_copy(dst, dst, sem).wait()

    def push(src, dst, send, recv, target):
        @pl.when(target == b)
        def _():
            pltpu.make_async_copy(src, dst, recv).start()

        @pl.when(target != b)
        def _():
            remote(src, dst, send, recv, (s, target, h)).start()

    def pushed(src, send, target):
        @pl.when(target != b)
        def _():
            remote(src, src, send, send, (s, target, h)).wait_send()

    barrier = pltpu.get_barrier_semaphore()
    for k in range(1, B):
        pl.semaphore_signal(barrier, inc=1, device_id=(s, ahead(k), h), device_id_type=MESH)
    pl.semaphore_signal(barrier, inc=1, device_id=(s, b, 1 - h), device_id_type=MESH)

    @pl.when(s > 0)
    def _():
        pl.semaphore_signal(barrier, inc=1, device_id=(s - 1, b, h), device_id_type=MESH)

    @pl.when(s < S - 1)
    def _():
        pl.semaphore_signal(barrier, inc=1, device_id=(s + 1, b, h), device_id_type=MESH)

    pl.semaphore_wait(barrier, B + (s > 0).astype(jnp.int32) + (s < S - 1).astype(jnp.int32))

    def row_block(c):
        return X.at[c, :, half]

    def col_block(j):
        return X.at[:, :, pl.ds(pl.multiple_of(h * width + j * hd, hd), hd)]

    swap_cores = lambda: remote(X.at[:, :, half], X.at[:, :, half], one.at[0], one.at[1], (s, b, 1 - h))
    swap_in = lambda: arrived(X.at[:, :, other_half], one.at[1])

    @pl.when(s == 0)
    def _():
        pltpu.make_async_copy(hid_in, row_block(b), one.at[2]).start()

    @pl.when(s == 1)
    def _():
        def hand_over(c, k):
            remote(G.at[c], row_block(c), gxs.at[k], yr.at[c], (s - 1, b, h)).start()

        for k in range(2, B, 2):
            remote(hid_in, G.at[b], gzs.at[k], gzr.at[b], (s, ahead(k), h)).start()
        remote(hid_in, G.at[b], gys.at[0], gyr.at[b], (s, mate, h)).start()
        for k in range(2, B, 2):
            c = ahead(k)
            arrived(G.at[c], gzr.at[c])
            remote(G.at[c], G.at[c], gys.at[k], gyr.at[c], (s, mate, h)).start()
            hand_over(c, k)
        for k in range(0, B, 2):
            c = lax.rem(mate + k, B)
            arrived(G.at[c], gyr.at[c])
            hand_over(c, k + 1)

    w_dst = W.at[:, pl.ds(pl.multiple_of(b * depth, depth), depth), :]
    st_dst = ST.at[:, b]

    def cols_of(j):
        return pl.ds(pl.multiple_of(j * hd, hd), hd)

    for k in range(heads):
        j = lax.rem(b + k, heads)
        push(w_in.at[:, :, cols_of(j)], w_dst, ws.at[k], wr.at[b], j + off)
    for k in range(heads):
        j = lax.rem(b + k, heads)
        push(stale_in.at[:, :, cols_of(j)], st_dst, ss.at[k], sr.at[b], j + off)

    def norm_states():
        values = X[...].reshape(total, 2 * width).astype(F32)
        XN[...] = rms(values, row_gain[...]).astype(BF16)

    @pl.when(s == 0)
    def _():
        pltpu.make_async_copy(hid_in, row_block(b), one.at[2]).wait()
        for k in range(1, B):
            arrived(row_block(ahead(k)), yr.at[ahead(k)])
        swap_cores().start()
        swap_in()

        @pl.when(owner)
        def _():
            norm_states()

    @pl.when(owner)
    def _():
        TN[...] = rms(text_in[...].astype(F32), row_gain[...]).astype(BF16)
        for c in range(B):
            arrived(W.at[:, pl.ds(c * depth, depth), :], wr.at[c])
        text_kv = jnp.dot(
            TN[...], jnp.concatenate([W[1], W[2]], axis=1), preferred_element_type=F32
        ).astype(BF16)
        TK[...] = rms(text_kv[:, :hd].astype(F32), head_gain[1:2, :]).astype(BF16)
        TV[...] = text_kv[:, hd:]

    @pl.when(s > 0)
    def _():
        @pl.when(owner)
        def _():
            mine = col_block(j_own)
            arrived(mine, one.at[3])
            for k in range(2, B, 2):
                remote(mine, mine, zs.at[k], zr.at[b], (s, ahead(k), h)).start()
            remote(mine, mine, ys.at[0], yr.at[b], (s, mate, h)).start()

        for k in range(2, B, 2):
            c = ahead(k)

            @pl.when((c >= off) & (c < off + heads))
            def _():
                block = col_block(c - off)
                arrived(block, zr.at[c])
                remote(block, block, ys.at[k], yr.at[c], (s, mate, h)).start()

        for k in range(0, B, 2):
            c = lax.rem(mate + k, B)

            @pl.when((c >= off) & (c < off + heads))
            def _():
                arrived(col_block(c - off), yr.at[c])

        swap_cores().start()
        swap_in()

        @pl.when(owner)
        def _():
            norm_states()

    @pl.when(owner)
    def _():
        proj = jnp.dot(
            XN[...], jnp.concatenate([W[0], W[1], W[2]], axis=1), preferred_element_type=F32
        )
        fresh_k = proj[:, hd : 2 * hd].astype(BF16)
        fresh_v = proj[:, 2 * hd :].astype(BF16)
        cache_own[0] = fresh_k.reshape(B, rows, hd)
        cache_own[1] = fresh_v.reshape(B, rows, hd)
        cols = cols_of(j_own)
        for k in range(B):
            t = ahead(k)
            push(cache_own.at[:, t], cache_out.at[:, :, cols], cs.at[k], cr.at[j_own], t)
        for c in range(B):
            arrived(ST.at[:, c], sr.at[c])
        tok_bits = tok.bit_length() - 1

        def place(shape, axis):
            at = lax.broadcasted_iota(jnp.int32, shape, axis)
            which = lax.shift_right_logical(at, tok_bits) & (micro - 1)
            spot = lax.shift_right_logical(at, rows.bit_length() - 1) * tok + (at & (tok - 1))
            return which, spot

        def per_micro(which, read):
            out = jnp.zeros(which.shape, jnp.int32)
            for m in range(micro):
                out = jnp.where(which == m, read(m), out)
            return out

        which, _ = place((total, hd), 0)
        use_stale = per_micro(which, lambda m: flags[s, m]) == 1
        kept_k = jnp.where(use_stale, ST[0].reshape(total, hd).astype(F32), fresh_k.astype(F32))
        kept_v = jnp.where(use_stale, ST[1].reshape(total, hd).astype(F32), fresh_v.astype(F32))
        keys = rms(kept_k, head_gain[1:2, :]).astype(BF16)
        queries = rms(proj[:, :hd], head_gain[0:1, :]).astype(BF16)
        scale = hd**-0.5
        nt = (((1,), (1,)), ((), ()))

        def attend(key_rows, value_rows, mask):
            scores = lax.dot_general(queries, key_rows, nt, preferred_element_type=F32) * scale
            probs = jnp.where(mask, jnp.exp(scores), 0.0)
            num = jnp.dot(probs.astype(BF16), value_rows, preferred_element_type=F32)
            return num, jnp.sum(probs, axis=1, keepdims=True)

        shape = (total, total)
        q_which, _ = place(shape, 0)
        k_which, k_spot = place(shape, 1)
        mask = (q_which == k_which) & (k_spot < per_micro(k_which, lambda m: patch_len[m]))
        num, den = attend(keys, kept_v.astype(BF16), mask)
        text_at = lax.broadcasted_iota(jnp.int32, (total, TK.shape[0]), 1)
        text_num, text_den = attend(TK[...], TV[...], text_at < text_len[0])
        attended = (num + text_num) / (den + text_den)
        state = X[:, :, pl.ds(pl.multiple_of(h * width + j_own * hd, hd), hd)]
        new = (state.reshape(total, hd).astype(F32) + attended).astype(BF16)
        hid_own[...] = new.reshape(B, rows, hd)

        @pl.when(s < S - 1)
        def _():
            remote(hid_own, col_block(j_own), one.at[4], one.at[3], (s + 1, b, h)).start()

        for k in range(B):
            t = ahead(k)
            push(hid_own.at[t], hid_out.at[:, cols], hs.at[k], hr.at[j_own], t)
        for k in range(B):
            t = ahead(k)
            pushed(hid_own.at[t], hs.at[k], t)
            pushed(cache_own.at[:, t], cs.at[k], t)

        @pl.when(s < S - 1)
        def _():
            remote(hid_own, col_block(j_own), one.at[4], one.at[3], (s + 1, b, h)).wait_send()

    for j in range(heads):
        cols = pl.ds(j * hd, hd)
        arrived(hid_out.at[:, cols], hr.at[j])
        arrived(cache_out.at[:, :, cols], cr.at[j])

    for k in range(heads):
        j = lax.rem(b + k, heads)
        pushed(w_in.at[:, :, cols_of(j)], ws.at[k], j + off)
        pushed(stale_in.at[:, :, cols_of(j)], ss.at[k], j + off)
    swap_cores().wait_send()

    @pl.when(s == 1)
    def _():
        for k in range(1, B):
            remote(G.at[b], G.at[b], gxs.at[k], gyr.at[b], (s - 1, b, h)).wait_send()
        for k in range(2, B, 2):
            remote(G.at[b], G.at[b], gzs.at[k], gzr.at[b], (s, ahead(k), h)).wait_send()
        for k in range(0, B, 2):
            remote(G.at[b], G.at[b], gys.at[k], gyr.at[b], (s, mate, h)).wait_send()

    @pl.when(s > 0)
    def _():
        block = col_block(0)

        @pl.when(owner)
        def _():
            for k in range(2, B, 2):
                remote(block, block, zs.at[k], zr.at[b], (s, ahead(k), h)).wait_send()

        for k in range(0, B, 2):
            c = ahead(k)

            @pl.when((c >= off) & (c < off + heads))
            def _():
                remote(block, block, ys.at[k], yr.at[b], (s, mate, h)).wait_send()


def shards(
    hidden_in, w_qkv, norm_gain, qk_gain, text_states, text_len, patch_len, stale_flags, stale_kv
):
    S, B = lax.axis_size("section"), lax.axis_size("blk")
    micro, tok, width = hidden_in.shape
    hd = qk_gain.shape[2]
    heads = width // hd
    rows = micro * tok
    total = B * rows
    depth = w_qkv.shape[1]
    text = text_states.shape[1]
    w = w_qkv[0].transpose(1, 0, 2)
    smem = pl.BlockSpec(memory_space=pltpu.SMEM)
    vmem = pl.BlockSpec(memory_space=pltpu.VMEM)
    sem = pltpu.SemaphoreType.DMA
    hid, cache = pl.pallas_call(
        functools.partial(kernel, (S, B, heads, hd, micro, tok)),
        out_shape=(
            jax.ShapeDtypeStruct((rows, width), BF16),
            jax.ShapeDtypeStruct((2, rows, width), BF16),
        ),
        in_specs=[smem] * 3 + [vmem] * 6,
        out_specs=(vmem, vmem),
        scratch_shapes=[
            pltpu.VMEM((B, rows, 2 * width), BF16),
            pltpu.VMEM((B, rows, width), BF16),
            pltpu.VMEM((total, 2 * width), BF16),
            pltpu.VMEM((text, 2 * width), BF16),
            pltpu.VMEM((3, B * depth, hd), BF16),
            pltpu.VMEM((2, B, rows, hd), BF16),
            pltpu.VMEM((text, hd), BF16),
            pltpu.VMEM((text, hd), BF16),
            pltpu.VMEM((B, rows, hd), BF16),
            pltpu.VMEM((2, B, rows, hd), BF16),
            sem((B,)), sem((B,)), sem((B,)), sem((B,)),
            sem((heads,)), sem((B,)), sem((heads,)), sem((B,)),
            sem((B,)), sem((heads,)), sem((B,)), sem((heads,)),
            sem((B,)), sem((B,)), sem((B,)), sem((B,)), sem((B + 1,)),
            sem((5,)),
        ],
        compiler_params=pltpu.CompilerParams(
            collective_id=0, has_side_effects=True, vmem_limit_bytes=60 * 1024 * 1024
        ),
    )(
        text_len, patch_len, stale_flags.T,
        hidden_in.reshape(rows, width), w, norm_gain, qk_gain[0], text_states[0],
        stale_kv[0].reshape(2, rows, width),
    )
    return (
        hid.reshape(1, micro, tok, width),
        cache.reshape(1, 2, micro, tok, width),
    )


def solution(mesh):
    in_specs = (
        P(None, "blk", "head"),
        P("section", "blk", None, "head"),
        P("section", None),
        P("section", None, None),
        P("section", None, None),
        P(),
        P(),
        P(),
        P("section", None, None, "blk", "head"),
    )
    out_specs = (P("section", None, "blk", "head"), P("section", None, None, "blk", "head"))
    return jax.shard_map(shards, mesh=mesh, in_specs=in_specs, out_specs=out_specs, check_vma=False)
```

```python
import functools

import jax
import jax.numpy as jnp
from jax import lax
from jax.experimental import pallas as pl
from jax.experimental.pallas import tpu as pltpu
from jax.sharding import PartitionSpec as P

MESH = pl.DeviceIdType.MESH
F32 = jnp.float32
BF16 = jnp.bfloat16


def rms(values, gain):
    return values * lax.rsqrt(jnp.mean(values * values, axis=-1, keepdims=True) + 1e-06) * gain


def kernel(
    dims,
    text_len, patch_len, flags,
    hid_in, w_in, row_gain, head_gain, text_hbm, stale_in,
    hid_out, cache_out,
    X, X1, RES, G, XN, text_in, TN, W, ST, TK, TV, hid_own, cache_own,
    zs, zr, ys, yr, ws, wr, ss, sr, hs, hr, cs, cr, gzs, gzr, gys, gyr, gxs, one,
):
    S, B, heads, hd, micro, tok = dims
    off = (B - heads) // 2
    rows = micro * tok
    total = B * rows
    width = heads * hd
    depth = w_in.shape[1]
    s, b, h = lax.axis_index("section"), lax.axis_index("blk"), lax.axis_index("head")
    mate = b + 1 - 2 * lax.rem(b, 2)
    j_own = b - off
    owner = (b >= off) & (b < off + heads)
    half = pl.ds(pl.multiple_of(h * width, hd), width)
    other_half = pl.ds(pl.multiple_of((1 - h) * width, hd), width)

    def ahead(k):
        return lax.rem(b + k, B)

    def remote(src, dst, send, recv, dev):
        return pltpu.make_async_remote_copy(
            src_ref=src, dst_ref=dst, send_sem=send, recv_sem=recv, device_id=dev, device_id_type=MESH
        )

    def arrived(dst, sem):
        pltpu.make_async_copy(dst, dst, sem).wait()

    def push(src, dst, send, recv, target):
        @pl.when(target == b)
        def _():
            pltpu.make_async_copy(src, dst, recv).start()

        @pl.when(target != b)
        def _():
            remote(src, dst, send, recv, (s, target, h)).start()

    def pushed(src, send, target):
        @pl.when(target != b)
        def _():
            remote(src, src, send, send, (s, target, h)).wait_send()

    text_copy = pltpu.make_async_copy(text_hbm, text_in, one.at[5])
    text_copy.start()
    barrier = pltpu.get_barrier_semaphore()
    for k in range(1, B):
        pl.semaphore_signal(barrier, inc=1, device_id=(s, ahead(k), h), device_id_type=MESH)
    pl.semaphore_signal(barrier, inc=1, device_id=(s, b, 1 - h), device_id_type=MESH)

    @pl.when(s > 0)
    def _():
        pl.semaphore_signal(barrier, inc=1, device_id=(s - 1, b, h), device_id_type=MESH)

    @pl.when(s < S - 1)
    def _():
        pl.semaphore_signal(barrier, inc=1, device_id=(s + 1, b, h), device_id_type=MESH)

    pl.semaphore_wait(barrier, B + (s > 0).astype(jnp.int32) + (s < S - 1).astype(jnp.int32))

    def row_block(c):
        return X.at[c, :, half]

    def col_block(j):
        return X1.at[h, j]

    def swap_cores():
        return remote(X.at[:, :, half], X.at[:, :, half], one.at[0], one.at[1], (s, b, 1 - h))

    def swap_blocks():
        return remote(X1.at[h], X1.at[h], one.at[0], one.at[1], (s, b, 1 - h))

    @pl.when(s == 0)
    def _():
        pltpu.make_async_copy(hid_in, row_block(b), one.at[2]).start()

    @pl.when(s == 1)
    def _():
        for k in range(2, B, 2):
            remote(hid_in, G.at[b], gzs.at[k], gzr.at[b], (s, ahead(k), h)).start()
        remote(hid_in, G.at[b], gys.at[0], gyr.at[b], (s, mate, h)).start()

    def hand_over(c, k):
        remote(G.at[c], row_block(c), gxs.at[k], yr.at[c], (s - 1, b, h)).start()

    @pl.when(s == 1)
    def _():
        for k in range(2, B, 2):
            c = ahead(k)
            arrived(G.at[c], gzr.at[c])
            remote(G.at[c], G.at[c], gys.at[k], gyr.at[c], (s, mate, h)).start()
            hand_over(c, k)

    w_dst = W.at[:, pl.ds(pl.multiple_of(b * depth, depth), depth), :]
    st_dst = ST.at[:, b]

    def cols_of(j):
        return pl.ds(pl.multiple_of(j * hd, hd), hd)

    for k in range(heads):
        j = lax.rem(b + k, heads)
        push(w_in.at[:, :, cols_of(j)], w_dst, ws.at[k], wr.at[b], j + off)
    for k in range(heads):
        j = lax.rem(b + k, heads)
        push(stale_in.at[:, :, cols_of(j)], st_dst, ss.at[k], sr.at[b], j + off)

    @pl.when(s == 1)
    def _():
        for k in range(0, B, 2):
            c = lax.rem(mate + k, B)
            arrived(G.at[c], gyr.at[c])
            hand_over(c, k + 1)

    def norm_states(values):
        values = values.astype(F32)
        XN[...] = rms(values, row_gain[...]).astype(BF16)

    @pl.when(s == 0)
    def _():
        pltpu.make_async_copy(hid_in, row_block(b), one.at[2]).wait()
        for k in range(1, B):
            arrived(row_block(ahead(k)), yr.at[ahead(k)])
        swap_cores().start()
        arrived(X.at[:, :, other_half], one.at[1])

        @pl.when(owner)
        def _():
            norm_states(X[...].reshape(total, 2 * width))
            RES[...] = X[:, :, pl.ds(pl.multiple_of(h * width + j_own * hd, hd), hd)].reshape(total, hd)

    text_copy.wait()

    @pl.when(owner)
    def _():
        TN[...] = rms(text_in[...].astype(F32), row_gain[...]).astype(BF16)
        for c in range(B):
            arrived(W.at[:, pl.ds(c * depth, depth), :], wr.at[c])
        text_kv = jnp.dot(
            TN[...], jnp.concatenate([W[1], W[2]], axis=1), preferred_element_type=F32
        ).astype(BF16)
        TK[...] = rms(text_kv[:, :hd].astype(F32), head_gain[1:2, :]).astype(BF16)
        TV[...] = text_kv[:, hd:]

    @pl.when(s > 0)
    def _():
        @pl.when(owner)
        def _():
            mine = col_block(j_own)
            arrived(mine, one.at[3])
            for k in range(2, B, 2):
                remote(mine, mine, zs.at[k], zr.at[b], (s, ahead(k), h)).start()
            remote(mine, mine, ys.at[0], yr.at[b], (s, mate, h)).start()

        for k in range(2, B, 2):
            c = ahead(k)

            @pl.when((c >= off) & (c < off + heads))
            def _():
                block = col_block(c - off)
                arrived(block, zr.at[c])
                remote(block, block, ys.at[k], yr.at[c], (s, mate, h)).start()

        for k in range(0, B, 2):
            c = lax.rem(mate + k, B)

            @pl.when((c >= off) & (c < off + heads))
            def _():
                arrived(col_block(c - off), yr.at[c])

        swap_blocks().start()
        arrived(X1.at[1 - h], one.at[1])

        @pl.when(owner)
        def _():
            norm_states(
                jnp.concatenate([X1[i, j] for i in range(2) for j in range(heads)], axis=1)
            )
            RES[...] = X1[h, j_own]

    @pl.when(owner)
    def _():
        proj = jnp.dot(
            XN[...], jnp.concatenate([W[0], W[1], W[2]], axis=1), preferred_element_type=F32
        )
        fresh_k = proj[:, hd : 2 * hd].astype(BF16)
        fresh_v = proj[:, 2 * hd :].astype(BF16)
        cache_own[0] = fresh_k.reshape(B, rows, hd)
        cache_own[1] = fresh_v.reshape(B, rows, hd)
        cols = cols_of(j_own)
        for k in range(B):
            t = ahead(k)
            push(cache_own.at[:, t], cache_out.at[:, :, cols], cs.at[k], cr.at[j_own], t)
        for c in range(B):
            arrived(ST.at[:, c], sr.at[c])
        tok_bits = tok.bit_length() - 1

        def place(shape, axis):
            at = lax.broadcasted_iota(jnp.int32, shape, axis)
            which = lax.shift_right_logical(at, tok_bits) & (micro - 1)
            spot = lax.shift_right_logical(at, rows.bit_length() - 1) * tok + (at & (tok - 1))
            return which, spot

        def per_micro(which, read):
            out = jnp.zeros(which.shape, jnp.int32)
            for m in range(micro):
                out = jnp.where(which == m, read(m), out)
            return out

        which, _ = place((total, hd), 0)
        use_stale = per_micro(which, lambda m: flags[s, m]) == 1
        kept_k = jnp.where(use_stale, ST[0].reshape(total, hd).astype(F32), fresh_k.astype(F32))
        kept_v = jnp.where(use_stale, ST[1].reshape(total, hd).astype(F32), fresh_v.astype(F32))
        keys = rms(kept_k, head_gain[1:2, :]).astype(BF16)
        queries = rms(proj[:, :hd], head_gain[0:1, :]).astype(BF16)
        scale = hd**-0.5
        nt = (((1,), (1,)), ((), ()))

        def attend(key_rows, value_rows, mask):
            scores = lax.dot_general(queries, key_rows, nt, preferred_element_type=F32) * scale
            probs = jnp.where(mask, jnp.exp(scores), 0.0)
            num = jnp.dot(probs.astype(BF16), value_rows, preferred_element_type=F32)
            return num, jnp.sum(probs, axis=1, keepdims=True)

        shape = (total, total)
        q_which, _ = place(shape, 0)
        k_which, k_spot = place(shape, 1)
        mask = (q_which == k_which) & (k_spot < per_micro(k_which, lambda m: patch_len[m]))
        num, den = attend(keys, kept_v.astype(BF16), mask)
        text_at = lax.broadcasted_iota(jnp.int32, (total, TK.shape[0]), 1)
        text_num, text_den = attend(TK[...], TV[...], text_at < text_len[0])
        attended = (num + text_num) / (den + text_den)
        hid_own[...] = (RES[...].astype(F32) + attended).astype(BF16)

        @pl.when(s < S - 1)
        def _():
            remote(hid_own, col_block(j_own), one.at[4], one.at[3], (s + 1, b, h)).start()

        for k in range(B):
            t = ahead(k)
            push(hid_own.at[pl.ds(pl.multiple_of(t * rows, rows), rows), :], hid_out.at[:, cols], hs.at[k], hr.at[j_own], t)
        for k in range(B):
            t = ahead(k)
            pushed(hid_own.at[pl.ds(0, rows), :], hs.at[k], t)
            pushed(cache_own.at[:, t], cs.at[k], t)

        @pl.when(s < S - 1)
        def _():
            remote(hid_own, col_block(j_own), one.at[4], one.at[3], (s + 1, b, h)).wait_send()

    for j in range(heads):
        cols = pl.ds(j * hd, hd)
        arrived(hid_out.at[:, cols], hr.at[j])
        arrived(cache_out.at[:, :, cols], cr.at[j])

    for k in range(heads):
        j = lax.rem(b + k, heads)
        pushed(w_in.at[:, :, cols_of(j)], ws.at[k], j + off)
        pushed(stale_in.at[:, :, cols_of(j)], ss.at[k], j + off)
    swap_cores().wait_send()

    @pl.when(s == 1)
    def _():
        for k in range(1, B):
            remote(G.at[b], G.at[b], gxs.at[k], gyr.at[b], (s - 1, b, h)).wait_send()
        for k in range(2, B, 2):
            remote(G.at[b], G.at[b], gzs.at[k], gzr.at[b], (s, ahead(k), h)).wait_send()
        for k in range(0, B, 2):
            remote(G.at[b], G.at[b], gys.at[k], gyr.at[b], (s, mate, h)).wait_send()

    @pl.when(s > 0)
    def _():
        block = col_block(0)

        @pl.when(owner)
        def _():
            for k in range(2, B, 2):
                remote(block, block, zs.at[k], zr.at[b], (s, ahead(k), h)).wait_send()

        for k in range(0, B, 2):
            c = ahead(k)

            @pl.when((c >= off) & (c < off + heads))
            def _():
                remote(block, block, ys.at[k], yr.at[b], (s, mate, h)).wait_send()


def shards(
    hidden_in, w_qkv, norm_gain, qk_gain, text_states, text_len, patch_len, stale_flags, stale_kv
):
    S, B = lax.axis_size("section"), lax.axis_size("blk")
    micro, tok, width = hidden_in.shape
    hd = qk_gain.shape[2]
    heads = width // hd
    rows = micro * tok
    total = B * rows
    depth = w_qkv.shape[1]
    text = text_states.shape[1]
    w = w_qkv[0].transpose(1, 0, 2)
    smem = pl.BlockSpec(memory_space=pltpu.SMEM)
    vmem = pl.BlockSpec(memory_space=pltpu.VMEM)
    hbm = pl.BlockSpec(memory_space=pl.ANY)
    sem = pltpu.SemaphoreType.DMA
    hid, cache = pl.pallas_call(
        functools.partial(kernel, (S, B, heads, hd, micro, tok)),
        out_shape=(
            jax.ShapeDtypeStruct((rows, width), BF16),
            jax.ShapeDtypeStruct((2, rows, width), BF16),
        ),
        in_specs=[smem] * 3 + [vmem, hbm, vmem, vmem, hbm, vmem],
        out_specs=(vmem, vmem),
        scratch_shapes=[
            pltpu.VMEM((B, rows, 2 * width), BF16),
            pltpu.VMEM((2, heads, total, hd), BF16),
            pltpu.VMEM((total, hd), BF16),
            pltpu.VMEM((B, rows, width), BF16),
            pltpu.VMEM((total, 2 * width), BF16),
            pltpu.VMEM((text, 2 * width), BF16),
            pltpu.VMEM((text, 2 * width), BF16),
            pltpu.VMEM((3, B * depth, hd), BF16),
            pltpu.VMEM((2, B, rows, hd), BF16),
            pltpu.VMEM((text, hd), BF16),
            pltpu.VMEM((text, hd), BF16),
            pltpu.VMEM((total, hd), BF16),
            pltpu.VMEM((2, B, rows, hd), BF16),
            sem((B,)), sem((B,)), sem((B,)), sem((B,)),
            sem((heads,)), sem((B,)), sem((heads,)), sem((B,)),
            sem((B,)), sem((heads,)), sem((B,)), sem((heads,)),
            sem((B,)), sem((B,)), sem((B,)), sem((B,)), sem((B + 1,)),
            sem((6,)),
        ],
        compiler_params=pltpu.CompilerParams(
            collective_id=0, has_side_effects=True, vmem_limit_bytes=60 * 1024 * 1024
        ),
    )(
        text_len, patch_len, stale_flags.T,
        hidden_in.reshape(rows, width), w, norm_gain, qk_gain[0], text_states[0],
        stale_kv[0].reshape(2, rows, width),
    )
    return (
        hid.reshape(1, micro, tok, width),
        cache.reshape(1, 2, micro, tok, width),
    )


def solution(mesh):
    in_specs = (
        P(None, "blk", "head"),
        P("section", "blk", None, "head"),
        P("section", None),
        P("section", None, None),
        P("section", None, None),
        P(),
        P(),
        P(),
        P("section", None, None, "blk", "head"),
    )
    out_specs = (P("section", None, "blk", "head"), P("section", None, None, "blk", "head"))
    return jax.shard_map(shards, mesh=mesh, in_specs=in_specs, out_specs=out_specs, check_vma=False)
```
